256 devices in a mesh: groups: 2 (over y), ep: 128 (over x, z, core).
Axes of the slice: x: 4, y: 2, z: 16, core: 2. Of those that a mesh axis runs over, the one named last changes fastest.
The devices are a block of a 4x16x16 slice.
Arguments:
- tokens: bfloat16 [4096, 2880], P(('groups', 'ep')), parts along dimension 0, may hold values from -6 to 6
- routes: int32 [4096, 4], P(('groups', 'ep')), parts along dimension 0, may hold values from 0 to 63, all different within a row; in each aligned block of 16 rows (0 to 15, 16 to 31, ...) at most 2 rows name the same one
- gate_fixed: int32 [4096, 4], P(('groups', 'ep')), parts along dimension 0, may hold values from 1 to 65535
- gate_weight: bfloat16 [128, 2880, 720], P('ep'), may hold values from -0.109375 to 0.109375
- up_weight: bfloat16 [128, 2880, 720], P('ep'), may hold values from -0.109375 to 0.109375
- down_weight: bfloat16 [128, 720, 2880], P('ep'), may hold values from -0.15625 to 0.15625
Outputs:
- mixed: bfloat16 [4096, 2880], P(('groups', 'ep')), parts along dimension 0
The draws below stay inside these ranges and needn't reach their ends.
There are 2 independent parts, one for each index of `groups`. The reference program is written for one: setup_inputs(seed, part) draws one part's arguments, and reference() takes and returns one part's arrays. A program takes and returns all parts, laid end to end along the dimension named above; an argument that names none is the same for every part. Nothing has to cross between parts.
Inputs may be any that keep to these rules, and one draw needn't show every extreme that they name: `routes`: each row names 4 different experts; the 16 rows of one device name any one expert at most 2 times.
All inputs are finite; a program needn't handle non-finite values.
Results may differ from the reference program's by a relative error of at most 0.0065.
Values may be sent and summed in bfloat16 or wider, within the bound.
A program may use at most 64 MiB of HBM per device.

```python
import math
import jax
import jax.numpy as jnp
import numpy as np
from jax import lax

D = 2880
FF = 1440
TOP = 4
TOK_DEV = 16
HALF = 720
EXPERTS = 64
TOKENS = 2048
CAP = 2
N_EP = 128


def set_ends(values, stream_key, least, high):
    longest = values.shape.index(max(values.shape))
    spots = []
    for shift in (0, 1):
        where = [jax.random.randint(jax.random.fold_in(stream_key, axis), (), 0, length) for axis, length in enumerate(values.shape)]
        where[longest] = (where[longest] + shift) % values.shape[longest]
        spots.append(tuple(where))
    return values.at[spots[0]].set(least).at[spots[1]].set(high)


def block_levels(rng, extent, split, least, top_value):
    level, own = 1.0, jax.random.fold_in(rng, 6)
    for dim, parts in split:
        steps = jnp.exp(jax.random.uniform(jax.random.fold_in(own, dim), (parts,), jnp.float32, least / len(split), top_value / len(split)))
        level = level * jnp.repeat(steps, extent[dim] // parts).reshape([-1 if axis == dim else 1 for axis in range(len(extent))])
    return level


def shared_out(stream_key, own, number, rows, amount, top, reach, lean):
    sequence = jax.random.permutation(stream_key, amount)
    heavy_load, ordinary = shares(amount, rows * top, reach, lean, True), shares(amount, rows * top, reach, lean, False)
    places = jnp.arange(amount)

    def named(lengths, turn):
        used = int((lengths > 0).sum())
        fixed = max(1, used // 4)
        moved = fixed + (places - fixed + turn * (used - fixed)) % max(1, amount - fixed)
        return jnp.zeros((amount,), jnp.int32).at[sequence[jnp.where(places < fixed, places, moved)]].set(jnp.asarray(lengths, jnp.int32))

    lengths = jnp.where(number % 4 == 0, named(heavy_load, number // 4), named(ordinary, number - number // 4 - 1))
    mixed = jax.random.permutation(jax.random.fold_in(own, 3), amount)
    giver, receiver = mixed[0:amount // 2 * 2:2], mixed[1:amount // 2 * 2:2]
    margin = jnp.minimum(lengths[giver] - 1, reach - lengths[receiver]) // 2
    margin = jnp.where((giver == sequence[0]) | (receiver == sequence[0]) | (lengths[receiver] == 0), 0, jnp.maximum(margin, 0))
    moved = jax.random.randint(jax.random.fold_in(own, 4), (amount // 2,), 0, 1 << 20) % (margin + 1)
    lengths = lengths.at[giver].add(-moved).at[receiver].add(moved)
    members = jnp.searchsorted(jnp.cumsum(lengths), jnp.arange(rows * top), side="right").astype(jnp.int32)
    grid = members.reshape(top, rows).T
    grid = grid[jax.random.permutation(jax.random.fold_in(own, 1), rows)]
    turn = jax.random.randint(jax.random.fold_in(own, 2), (rows, 1), 0, top)
    return jnp.take_along_axis(grid, (jnp.arange(top)[None, :] + turn) % top, axis=1)


def shares(count, total, limit, lean, full):
    weights = [(1 << 20) // math.isqrt(standing ** lean) + 1 for standing in range(1, count + 1)]
    largest = limit if full else min(limit, max(-(-total // count), total * weights[0] // sum(weights)))
    least = 1 if total - largest >= count - 1 else 0
    given, surplus = [largest] + [least] * (count - 1), total - largest - least * (count - 1)
    while surplus > 0:
        free = [i for i in range(1, count) if given[i] < largest] or [i for i in range(1, count) if given[i] < limit]
        pool, budget = sum([weights[i] for i in free]), surplus
        for i in free:
            more = min(limit - given[i], max(1, budget * weights[i] // pool), surplus)
            given[i] = given[i] + more
            surplus = surplus - more
    return np.array(given)


def noise(own_key, dims, spread, limit, shards=(), kind=jnp.bfloat16):
    drawn = jax.random.normal(own_key, dims, jnp.float32) * spread
    if len(shards) > 0:
        drawn = block_levels(own_key, dims, shards, -0.22, 0.18) * drawn
    return jnp.clip(drawn, min=-limit, max=limit).astype(kind)


def setup_inputs(seed: int = 0, part: int = 0) -> dict:
    streams_of = jax.random.split(jax.random.key(seed), 7)
    part_keys = jax.random.split(jax.random.fold_in(streams_of[6], part), 7)
    tokens = noise(part_keys[0], (TOKENS, D), 1.0, 6.0, ((0, 128),))
    routes_keys = jax.random.split(jax.random.fold_in(part_keys[1], 1), TOKENS // TOK_DEV)
    routes_turns = jax.random.permutation(jax.random.fold_in(part_keys[1], 3), TOKENS // TOK_DEV)
    routes = jax.vmap(lambda own, number: shared_out(jax.random.fold_in(part_keys[1], 2), own, number, TOK_DEV, EXPERTS, TOP, CAP, 2))(routes_keys, routes_turns).reshape((TOKENS, TOP))
    gate_fixed = set_ends(jax.random.randint(part_keys[2], (TOKENS, TOP), 1, 65536), jax.random.fold_in(part_keys[2], 1), 1, 65535).astype(jnp.int32)
    gate_weight = noise(streams_of[3], (N_EP, D, HALF), D ** -0.5, 0.109375, ((0, 128),))
    up_weight = noise(streams_of[4], (N_EP, D, HALF), D ** -0.5, 0.109375, ((0, 128),))
    down_weight = noise(streams_of[5], (N_EP, HALF, D), FF ** -0.5, 0.15625, ((0, 128),))
    return dict(tokens=tokens, routes=routes, gate_fixed=gate_fixed, gate_weight=gate_weight, up_weight=up_weight, down_weight=down_weight)


def reference(tokens, routes, gate_fixed, gate_weight, up_weight, down_weight):
    experts = N_EP // 2
    onehot = (routes[:, :, None] == jnp.arange(experts, dtype=jnp.int32)).astype(jnp.int32)
    grouped = onehot.reshape(N_EP, TOK_DEV * TOP, experts)
    before = jnp.cumsum(grouped, axis=1) - grouped
    position = jnp.sum(before * grouped, axis=-1).reshape(TOKENS, TOP).astype(jnp.int32)
    source = (jnp.arange(TOKENS, dtype=jnp.int32) // TOK_DEV)[:, None]
    column = (source * CAP + position).astype(jnp.int32)
    token_ids = jnp.broadcast_to(jnp.arange(TOKENS, dtype=jnp.int32)[:, None], (TOKENS, TOP))
    slot_table = jnp.full((experts, N_EP * CAP), TOKENS, jnp.int32).at[routes, column].set(token_ids)
    padded = jnp.concatenate([tokens, jnp.zeros((1, D), tokens.dtype)], axis=0)

    def half_part(expert_rows, index):
        w_gate = lax.dynamic_index_in_dim(gate_weight, index, 0, keepdims=False)
        w_up = lax.dynamic_index_in_dim(up_weight, index, 0, keepdims=False)
        w_down = lax.dynamic_index_in_dim(down_weight, index, 0, keepdims=False)
        gate_part = jnp.dot(expert_rows, w_gate, preferred_element_type=jnp.float32)
        up_part = jnp.dot(expert_rows, w_up, preferred_element_type=jnp.float32)
        hidden = (jax.nn.silu(gate_part) * up_part).astype(jnp.bfloat16)
        return jnp.dot(hidden, w_down, preferred_element_type=jnp.float32).astype(jnp.bfloat16)

    def run_expert(expert):
        expert_rows = padded[slot_table[expert]]
        first = (2 * expert).astype(jnp.int32)
        lower = half_part(expert_rows, first)
        upper = half_part(expert_rows, (first + 1).astype(jnp.int32))
        return (lower.astype(jnp.float32) + upper.astype(jnp.float32)).astype(jnp.bfloat16)

    outputs = lax.map(run_expert, jnp.arange(experts, dtype=jnp.int32))
    picked = outputs[routes, column]
    weights = gate_fixed.astype(jnp.float32) / 65536.0
    mixed = jnp.sum(weights[:, :, None] * picked.astype(jnp.float32), axis=1)
    return mixed.astype(jnp.bfloat16)
```

```python
import functools

import jax
import jax.numpy as jnp
from jax import lax
from jax.experimental import pallas as pl
from jax.experimental.pallas import tpu as pltpu
from jax.sharding import PartitionSpec as P

MESH = pl.DeviceIdType.MESH
LANES = 128
CHUNKS = 2
PARTS = 3
BLOCKS = 8


def ring_sizes(mesh):
    row = mesh.devices.reshape(-1, mesh.devices.shape[-1])[0]
    coords = [tuple(d.coords) for d in row]
    cores = coords.count(coords[0])
    across = len({c[0] for c in coords})
    return across, len(row) // (across * cores), cores


def slot_of(way, hop, ring):
    if hop == 0:
        return 0
    if 2 * hop == ring:
        return ring - 1
    return 2 * hop - 1 + way


def kernel(across, ring, tok_hbm, meta_ref, wg_hbm, wu_hbm, wd_hbm, out_ref, tok, gathered, wg, wu, wd,
           select_out, rows_in, part, half_out, half_in, expert_out, returned, combined, sum_in, sum_out,
           load_sem, ag_send, ag_recv, xd_send, xd_recv, fw_send, fw_recv, hp_send, hp_recv,
           xr_send, xr_recv, rs_send, rs_recv):
    count, width = tok.shape
    wide = gathered.shape[2]
    groups = ring // BLOCKS
    held = BLOCKS * count
    reach = ring // 2
    me = lax.axis_index("ep")
    core = lax.rem(me, 2)
    z = lax.rem(me // 2, ring)
    x = me // (2 * ring)

    def at(xx, zz, cc):
        return {"ep": (lax.rem(xx + across, across) * ring + lax.rem(zz + ring, ring)) * 2 + cc}

    ends = (at(x, z + 1, core), at(x, z - 1, core))
    partner = at(x, z, 1 - core)
    sides = [at(x + d, z, core) for d in range(across)]

    tok_load = pltpu.make_async_copy(tok_hbm, tok, load_sem.at[0])
    tok_load.start()
    loads = [pltpu.make_async_copy(s, d, load_sem.at[i + 1])
             for i, (s, d) in enumerate(((wg_hbm, wg), (wu_hbm, wu), (wd_hbm, wd)))]
    barrier = pltpu.get_barrier_semaphore()
    friends = list(ends) + [partner] + sides[1:]
    for friend in friends:
        pl.semaphore_signal(barrier, inc=1, device_id=friend, device_id_type=MESH)
    tok_load.wait()
    gathered[0, :, pl.ds(0, wide - LANES)] = tok[:, pl.ds(0, wide - LANES)]
    tail = width - (wide - LANES)
    gathered[0, :, pl.ds(wide - LANES, tail)] = tok[:, pl.ds(wide - LANES, tail)]
    gathered[0, :, pl.ds(width, LANES - tail)] = meta_ref[:, pl.ds(tail, LANES - tail)]
    pl.semaphore_wait(barrier, len(friends))
    for load in loads:
        load.start()

    edges = [((wide // LANES) * i + CHUNKS - 1) // CHUNKS * LANES for i in range(CHUNKS + 1)]
    spans = [(edges[i], edges[i + 1]) for i in range(CHUNKS)]

    def span(ref, c, full):
        low, high = spans[c]
        return ref.at[:, pl.ds(low, min(high, full) - low)]

    def carries(way, hop, c):
        return hop < reach or (2 * c < CHUNKS) == (way == 0)

    def gather_copy(way, hop, c):
        return pltpu.make_async_remote_copy(
            span(gathered.at[slot_of(way, hop - 1, ring)], c, wide),
            span(gathered.at[slot_of(way, hop, ring)], c, wide),
            ag_send.at[way, hop - 1, c], ag_recv.at[way, hop - 1, c],
            device_id=ends[way], device_id_type=MESH)

    def gather_hop(hop):
        for c in range(CHUNKS):
            for way in range(2):
                if 1 < hop and carries(way, hop - 1, c):
                    gather_copy(way, hop - 1, c).wait_recv()
                if hop <= reach and carries(way, hop, c):
                    gather_copy(way, hop, c).start()

    lane = lax.broadcasted_iota(jnp.int32, (held, LANES), 1)
    token_row = lax.broadcasted_iota(jnp.int32, (held, LANES), 0)
    piece = 2 * BLOCKS
    half_lanes = across * piece
    inner = lax.rem(lane, half_lanes)
    target = lax.rem(inner // piece + x, across)
    wanted = ((target * ring + z) * 2 + lax.rem(inner, 2)).astype(jnp.float32)
    own_block = lax.rem(inner, piece) // 2 == token_row // count
    first_half = lane < half_lanes

    def matches(g):
        meta = gathered[pl.ds(g * BLOCKS, BLOCKS), :, pl.ds(wide - LANES, LANES)]
        return meta.reshape(held, LANES).astype(jnp.float32)

    def choose(g):
        meta = matches(g)
        sel = jnp.zeros((held, LANES), jnp.float32)
        for k in range(4):
            hit = (meta[:, tail + k:tail + k + 1] == wanted) & own_block
            sel = sel + jnp.where(hit, 1.0, 0.0)
        sel_t = sel.T[:half_lanes].astype(jnp.bfloat16)
        data = gathered[pl.ds(g * BLOCKS, BLOCKS), :, pl.ds(0, width)].reshape(held, width)
        picked = jnp.dot(sel_t, data, preferred_element_type=jnp.float32).astype(jnp.bfloat16)
        select_out[g] = picked.reshape(across, piece, width)
        rows_in[g, 0, 0] = picked[:piece]

    def dispatch_copy(g, d):
        return pltpu.make_async_remote_copy(
            select_out.at[g, d], rows_in.at[g, 0, d], xd_send.at[g, d], xd_recv.at[g, d],
            device_id=sides[d], device_id_type=MESH)

    def share_copy(g, d):
        source = select_out.at[g, 0] if d == 0 else rows_in.at[g, 0, d]
        return pltpu.make_async_remote_copy(
            source, rows_in.at[g, 1, d], fw_send.at[g, d], fw_recv.at[g, d],
            device_id=partner, device_id_type=MESH)

    order = [d for d in range(1, across) if d != across // 2] + ([across // 2] if across > 1 else [])

    def dispatch(g):
        choose(g)
        for d in order:
            dispatch_copy(g, d).start()
        share_copy(g, 0).start()

    def share(g):
        for d in order:
            dispatch_copy(g, d).wait_recv()
            share_copy(g, d).start()

    mine = across * piece

    def expert(g):
        for d in [0] + order:
            share_copy(g, d).wait_recv()

        part[g] = jnp.zeros(part.shape[1:], jnp.float32)

        @pl.loop(0, PARTS)
        def _(n):
            data = rows_in[g].reshape(2 * mine, width)
            contract = (((1,), (1,)), ((), ()))
            gate = lax.dot_general(data, wg[n], contract, preferred_element_type=jnp.float32)
            up = lax.dot_general(data, wu[n], contract, preferred_element_type=jnp.float32)
            hidden = (gate / (1.0 + jnp.exp(-gate)) * up).astype(jnp.bfloat16)
            part[g] += jnp.dot(hidden, wd[n], preferred_element_type=jnp.float32)

        half_out[g] = part[g, pl.ds(mine, mine)].astype(jnp.bfloat16)
        half_copy(g).start()

    def half_copy(g):
        return pltpu.make_async_remote_copy(
            half_out.at[g], half_in.at[g], hp_send.at[g], hp_recv.at[g],
            device_id=partner, device_id_type=MESH)

    def return_copy(g, d):
        return pltpu.make_async_remote_copy(
            expert_out.at[g, d], returned.at[g, d], xr_send.at[g, d], xr_recv.at[g, d],
            device_id=sides[(across - d) % across], device_id_type=MESH)

    def give_back(g):
        half_copy(g).wait_recv()
        total = (part[g, pl.ds(0, mine)] + half_in[g].astype(jnp.float32)).astype(jnp.bfloat16)
        expert_out[g] = total.reshape(across, piece, width)
        returned[g, 0] = total[:piece]
        for d in order:
            return_copy(g, d).start()

    def combine(g):
        meta = matches(g)
        mix = jnp.zeros((held, LANES), jnp.float32)
        for k in range(4):
            hit = (meta[:, tail + k:tail + k + 1] == wanted) & own_block
            high = meta[:, tail + 4 + k:tail + 5 + k] / 256.0
            low = meta[:, tail + 8 + k:tail + 9 + k] / 65536.0
            mix = mix + jnp.where(hit, jnp.where(first_half, high, low), 0.0)
        for d in order:
            return_copy(g, d).wait_recv()
        data = returned[g].reshape(mine, width)
        data = jnp.concatenate([data, data], axis=0)
        total = jnp.dot(mix.astype(jnp.bfloat16), data, preferred_element_type=jnp.float32)
        combined[pl.ds(g * BLOCKS, BLOCKS)] = total.reshape(BLOCKS, count, width)

    def sum_copy(way, hop, c):
        return pltpu.make_async_remote_copy(
            span(sum_out.at[way, hop - 1], c, width), span(sum_in.at[way, hop - 1], c, width),
            rs_send.at[way, hop - 1, c], rs_recv.at[way, hop - 1, c],
            device_id=ends[way], device_id_type=MESH)

    def sum_hop(hop):
        for c in range(CHUNKS):
            for way in range(2):
                if not carries(way, hop, c):
                    continue
                low, high = spans[c]
                high = min(high, width)
                value = combined[slot_of(1 - way, hop, ring), :, pl.ds(low, high - low)]
                if hop < reach and carries(way, hop + 1, c):
                    sum_copy(way, hop + 1, c).wait_recv()
                    value = value + sum_in[way, hop, :, pl.ds(low, high - low)].astype(jnp.float32)
                sum_out[way, hop - 1, :, pl.ds(low, high - low)] = value.astype(jnp.bfloat16)
                sum_copy(way, hop, c).start()

    complete = [max(h for h in range(reach + 1) for w in range(2) if slot_of(w, h, ring) < (g + 1) * BLOCKS)
                for g in range(groups)]
    for hop in range(1, reach + 2):
        gather_hop(hop)
        for g in range(groups):
            if complete[g] == hop - 1:
                dispatch(g)
            elif complete[g] == hop - 3:
                share(g)
    for load in loads:
        load.wait()
    for g in range(groups):
        if complete[g] > reach - 2:
            share(g)
        expert(g)
    for g in reversed(range(groups)):
        give_back(g)
    ready = groups
    for hop in range(reach, 0, -1):
        lowest = min(slot_of(w, hop, ring) for w in range(2)) // BLOCKS
        while ready > lowest:
            ready -= 1
            combine(ready)
        sum_hop(hop)
    for c in range(CHUNKS):
        low, high = spans[c]
        high = min(high, width)
        value = combined[0, :, pl.ds(low, high - low)]
        for way in range(2):
            sum_copy(way, 1, c).wait_recv()
            value = value + sum_in[way, 0, :, pl.ds(low, high - low)].astype(jnp.float32)
        out_ref[:, pl.ds(low, high - low)] = value.astype(jnp.bfloat16)

    for hop in range(1, reach + 1):
        for c in range(CHUNKS):
            for way in range(2):
                if carries(way, hop, c):
                    gather_copy(way, hop, c).wait_send()
                    sum_copy(way, hop, c).wait_send()
    for g in range(groups):
        for d in order:
            dispatch_copy(g, d).wait_send()
            return_copy(g, d).wait_send()
        for d in range(across):
            share_copy(g, d).wait_send()
        half_copy(g).wait_send()


def local(across, ring, tokens, routes, gate_fixed, gate_weight, up_weight, down_weight):
    count, width = tokens.shape
    top = routes.shape[1]
    hidden = gate_weight.shape[2]
    wide = -(-width // LANES) * LANES
    tail = width - (wide - LANES)
    earlier = jnp.arange(count)[:, None] > jnp.arange(count)[None, :]
    same = (routes[:, :, None, None] == routes[None, None, :, :]) & earlier[:, None, :, None]
    position = jnp.sum(same.astype(jnp.int32), axis=(2, 3))
    meta = jnp.concatenate([routes * 2 + position, gate_fixed // 256, gate_fixed % 256], axis=1)
    meta = jnp.pad(meta.astype(jnp.bfloat16), ((0, 0), (tail, LANES - tail - 3 * top)))
    groups = ring // BLOCKS
    reach = ring // 2
    piece = 2 * BLOCKS
    mine = across * piece
    held = BLOCKS * count
    bf16, f32 = jnp.bfloat16, jnp.float32
    dma = pltpu.SemaphoreType.DMA
    wg = jnp.swapaxes(gate_weight[0], 0, 1).reshape(PARTS, hidden // PARTS, width)
    wu = jnp.swapaxes(up_weight[0], 0, 1).reshape(PARTS, hidden // PARTS, width)
    wd = down_weight[0].reshape(PARTS, hidden // PARTS, width)
    vmem, anywhere = pl.BlockSpec(memory_space=pltpu.VMEM), pl.BlockSpec(memory_space=pl.ANY)
    return pl.pallas_call(
        functools.partial(kernel, across, ring),
        out_shape=jax.ShapeDtypeStruct((count, width), bf16),
        in_specs=[anywhere, vmem, anywhere, anywhere, anywhere],
        out_specs=vmem,
        scratch_shapes=[
            pltpu.VMEM((count, width), bf16),
            pltpu.VMEM((ring, count, wide), bf16),
            pltpu.VMEM(wg.shape, bf16),
            pltpu.VMEM(wu.shape, bf16),
            pltpu.VMEM(wd.shape, bf16),
            pltpu.VMEM((groups, across, piece, width), bf16),
            pltpu.VMEM((groups, 2, across, piece, width), bf16),
            pltpu.VMEM((groups, 2 * mine, width), f32),
            pltpu.VMEM((groups, mine, width), bf16),
            pltpu.VMEM((groups, mine, width), bf16),
            pltpu.VMEM((groups, across, piece, width), bf16),
            pltpu.VMEM((groups, across, piece, width), bf16),
            pltpu.VMEM((ring, count, width), f32),
            pltpu.VMEM((2, reach, count, width), bf16),
            pltpu.VMEM((2, reach, count, width), bf16),
            dma((4,)),
            dma((2, reach, CHUNKS)), dma((2, reach, CHUNKS)),
            dma((groups, across)), dma((groups, across)),
            dma((groups, across)), dma((groups, across)),
            dma((groups,)), dma((groups,)),
            dma((groups, across)), dma((groups, across)),
            dma((2, reach, CHUNKS)), dma((2, reach, CHUNKS)),
        ],
        compiler_params=pltpu.CompilerParams(
            collective_id=0, has_side_effects=True, vmem_limit_bytes=60 * 1024 * 1024
        ),
    )(tokens, meta, wg, wu, wd)


def solution(mesh):
    across, ring, _ = ring_sizes(mesh)
    placed = (
        P(("groups", "ep"), None),
        P(("groups", "ep"), None),
        P(("groups", "ep"), None),
        P("ep", None, None),
        P("ep", None, None),
        P("ep", None, None),
    )
    return jax.shard_map(
        functools.partial(local, across, ring),
        mesh=mesh, in_specs=placed, out_specs=P(("groups", "ep"), None), check_vma=False,
    )
```
